32 devices in a mesh: row: 8 (over z, core), col: 4 (over y, x).
Axes of the slice: x: 2, y: 2, z: 4, core: 2. Of those that a mesh axis runs over, the one named last changes fastest.
Arguments:
- genotypes: int32 [512, 16384], P(('row', 'col')), may hold values from 0 to 2, as said below
- snp_index: int32 [512], P(('row', 'col')), may hold values from 0 to 2047, as said below
- freq_table: float32 [2048], replicated, as said below
- prior: float32 [16384, 16384], P('row', 'col'), as said below
- start_vectors: float32 [16384, 20], P('row'), may hold values from -6 to 6
Outputs:
- grm: float32 [16384, 16384], P('row', 'col')
- pcs: float32 [16384, 20], P('col')
- spectrum: float32 [3, 20], replicated
The draws below stay inside these ranges and needn't reach their ends.
Inputs may be any that keep to these rules, and one draw needn't show every extreme that they name: `genotypes`: genotype dosages 0, 1 or 2. `snp_index`: strictly increasing; entry j lies in 4 * j to 4 * j + 3. `freq_table`: frequencies are multiples of 1/1024 between 52/1024 and 512/1024. `prior`: exactly symmetric; diagonal between 1 and 2, off-diagonal entries small.
All inputs are finite; a program needn't handle non-finite values.
Results may differ from the reference program's by a relative error of at most 0.0075.
Values may be sent and summed in bfloat16 or wider, within the bound.
A program may use at most 128 MiB of HBM per device.

```python
import jax
import jax.numpy as jnp
from jax import lax

S = 16384
M = 512
STRIDE = 4
K = 20
ITERS = 3


def window_plan(key):
    offsets = jax.random.randint(jax.random.fold_in(key, 11), (M,), 0, STRIDE)
    positions = jnp.arange(M, dtype=jnp.int32) * STRIDE + offsets.astype(jnp.int32)
    numerators = jax.random.randint(jax.random.fold_in(key, 12), (M * STRIDE,), 52, 513)
    return (positions.astype(jnp.int32), numerators.astype(jnp.int32))


def draw_snp_index(key, part):
    positions, numerators = window_plan(key)
    return positions


def draw_freq_table(key, part):
    positions, numerators = window_plan(key)
    return numerators.astype(jnp.float32) / 1024.0


def draw_genotypes(key, part):
    positions, numerators = window_plan(key)
    chosen = jnp.take(numerators, positions)[:, None]
    first = jax.random.randint(jax.random.fold_in(key, 13), (M, S), 0, 1024)
    second = jax.random.randint(jax.random.fold_in(key, 14), (M, S), 0, 1024)
    return (first < chosen).astype(jnp.int32) + (second < chosen).astype(jnp.int32)


def draw_prior(key, part):
    noise = jax.random.normal(jax.random.fold_in(key, 21), (S, S), jnp.float32)
    offdiag = (noise + noise.T) * 0.002
    diagonal = jax.random.uniform(jax.random.fold_in(key, 22), (S,), jnp.float32, 1.0, 2.0)
    places = jnp.arange(S)
    return offdiag.at[places, places].set(diagonal)


def block_scale(rng, dims, shards, low, high):
    loudness, own = 1.0, jax.random.fold_in(rng, 6)
    for dim, blocks in shards:
        steps = jnp.exp(jax.random.uniform(jax.random.fold_in(own, dim), (blocks,), jnp.float32, low / len(shards), high / len(shards)))
        loudness = loudness * jnp.repeat(steps, dims[dim] // blocks).reshape([-1 if axis == dim else 1 for axis in range(len(dims))])
    return loudness


def bell_draw(key, dims, scale, reach, split=(), held_as=jnp.bfloat16):
    drawn = scale * jax.random.normal(key, dims, jnp.float32)
    if split:
        drawn = drawn * block_scale(key, dims, split, -0.22, 0.18)
    return jnp.clip(drawn, -reach, reach).astype(held_as)


def setup_inputs(seed: int = 0) -> dict:
    seeds = jax.random.split(jax.random.key(seed), 6)
    return {
        "genotypes": draw_genotypes(jax.random.fold_in(seeds[5], 71), 0),
        "snp_index": draw_snp_index(jax.random.fold_in(seeds[5], 71), 0),
        "freq_table": draw_freq_table(jax.random.fold_in(seeds[5], 71), 0),
        "prior": draw_prior(jax.random.fold_in(seeds[5], 71), 0),
        "start_vectors": bell_draw(seeds[4], (S, K), 1.0, 6.0, ((0, 8),), jnp.float32),
    }


def standardize(genotypes, allele_freq):
    doubled = 2.0 * allele_freq
    spread = jnp.sqrt(doubled * (1.0 - allele_freq))
    return (genotypes.astype(jnp.float32) - doubled[:, None]) / spread[:, None]

def orthonormal(factor, image):
    return lax.linalg.triangular_solve(factor, image, left_side=False, lower=True, transpose_a=True)

def reference(genotypes, snp_index, freq_table, prior, start_vectors):
    allele_freq = jnp.take(freq_table, snp_index.astype(jnp.int32))
    standard = standardize(genotypes, allele_freq).astype(jnp.bfloat16)
    widened = lax.optimization_barrier(standard).astype(jnp.float32)
    window = jnp.dot(widened.T, widened, precision=lax.Precision.HIGHEST)
    grm = prior + window / M
    vectors = start_vectors / jnp.sqrt(jnp.float32(S))
    diagonals = []
    for step in range(ITERS):
        image = jnp.dot(grm, vectors, precision=lax.Precision.HIGHEST)
        gram = jnp.dot(image.T, image, precision=lax.Precision.HIGHEST)
        factor = jnp.linalg.cholesky(gram)
        diagonals.append(jnp.diagonal(factor))
        vectors = orthonormal(factor, image)
    pcs = vectors * jnp.sqrt(jnp.float32(S))
    spectrum = jnp.stack(diagonals, axis=0)
    return (grm, pcs, spectrum)
```

```python
import functools

import jax
import jax.numpy as jnp
from jax import lax
from jax.experimental import pallas as pl
from jax.experimental.pallas import tpu as pltpu
from jax.sharding import PartitionSpec as P

ITERS = 3
MESH = pl.DeviceIdType.MESH
SLOTS = 4
F32, BF16 = jnp.float32, jnp.bfloat16


def dot(a, b, dims=((1,), (0,)), precision=None):
    return lax.dot_general(
        a, b, (dims, ((), ())), precision=precision, preferred_element_type=jnp.float32
    )


ROWS = ((1,), (1,))


def loop(size, step, body):
    step = min(step, size)

    def one(j, carry):
        body(pl.ds(pl.multiple_of(j * step, step), step))
        return carry

    lax.fori_loop(0, size // step, one, 0)


def cholesky_inverse(gram, count):
    height = gram.shape[0]
    row = lax.broadcasted_iota(jnp.int32, (height, 128), 0)
    lane = lax.broadcasted_iota(jnp.int32, (height, 128), 1)
    eye = jnp.where(row == lane - height, 1.0, 0.0).astype(F32)
    both = jnp.concatenate([gram, jnp.zeros((height, 128 - height), F32)], axis=1) + eye
    diag = jnp.zeros((1, 128), F32)
    for k in range(count):
        pivot = both[k : k + 1, k : k + 1]
        inv = lax.rsqrt(pivot)
        head = both[k : k + 1, :] * inv
        below = jnp.where(row[:, :1] > k, both[:, k : k + 1] * inv, 0.0)
        both = jnp.where(row == k, head, both - below * head)
        diag = jnp.where(lane[:1, :] == k, pivot * inv, diag)
    return both[:, height : 2 * height], diag


def main_kernel(nr, nc, count, root, *refs):
    idx, freq, geno, start, prior, rp_out, cp_out, tile_out, pcs, spectrum = refs[:10]
    refs = refs[10:]
    rp, cp, std, tile, stage, acc, vec, image = refs[:8]
    stage_sem, out_sem = refs[8:10]
    s_row, r_row, s_col, r_col, s_acr, r_acr, s_rt, r_rt, s_lt, r_lt = refs[10:20]
    sums_a, sums_b = refs[20:34], refs[34:48]
    cs_land, s_cs, r_cs = refs[48:51]
    grams = refs[51:]

    row, col = lax.axis_index("row"), lax.axis_index("col")
    own, samples = std.shape
    depth, lr = rp.shape
    lc = cp.shape[1]
    height = vec.shape[0]
    nz = nr // 2
    core, zed = lax.rem(row, 2), lax.div(row, 2)
    scale = 1.0 / depth
    row_peers = [lax.rem(row + d, nr) for d in range(1, nr)]
    col_peers = [lax.rem(col + d, nc) for d in range(1, nc)]
    z_peers = [lax.rem(zed + d, nz) for d in range(1, nz)]
    partner = row + 1 - 2 * core

    barrier = pltpu.get_barrier_semaphore()
    for peer in row_peers:
        pl.semaphore_signal(barrier, inc=1, device_id={"row": peer}, device_id_type=MESH)
    for peer in col_peers:
        pl.semaphore_signal(barrier, inc=1, device_id={"col": peer}, device_id_type=MESH)

    def remote(src, dst, send_sem, recv_sem, target):
        return pltpu.make_async_remote_copy(
            src_ref=src,
            dst_ref=dst,
            send_sem=send_sem,
            recv_sem=recv_sem,
            device_id=target,
            device_id_type=MESH,
        )

    band = stage.shape[1]
    bands = lr // band

    def fetch(i):
        return pltpu.make_async_copy(
            prior.at[pl.ds(i * band, band)], stage.at[i % SLOTS], stage_sem.at[i % SLOTS]
        )

    for i in range(min(SLOTS, bands)):
        fetch(i).start()

    place = lax.broadcasted_iota(jnp.int32, (own, 1), 0)
    allele = jnp.zeros((own, 1), F32)
    for j in range(own):
        allele = jnp.where(place == j, freq[idx[j]], allele)
    doubled = 2.0 * allele
    spread = jnp.sqrt(doubled * (1.0 - allele))
    levels = [(float(g) - doubled) / spread for g in range(3)]

    def standardize(part):
        g = geno[:, part]
        value = jnp.where(g == 0, levels[0], jnp.where(g == 1, levels[1], levels[2]))
        std[:, part] = value.astype(BF16)

    loop(samples, 2048, standardize)
    vec[...] = jnp.concatenate(
        [start[...] * (1.0 / root), jnp.zeros((height - count, lr), F32)], axis=0
    ).astype(BF16)

    pl.semaphore_wait(barrier, nr + nc - 2)

    def cut(index, length):
        return std.at[:, pl.ds(pl.multiple_of(index * length, 128), length)]

    def piece(panel, r, q):
        return panel.at[pl.ds(pl.multiple_of((r * nc + q) * own, own), own)]

    by_col = [
        remote(cut(peer, lc), piece(cp, row, col), s_col.at[d], r_col.at[d], {"col": peer})
        for d, peer in enumerate(col_peers)
    ]
    for copy in by_col:
        copy.start()
    piece(cp, row, col)[...] = cut(col, lc)[...]
    piece(rp, row, col)[...] = cut(row, lr)[...]

    by_row = [
        remote(cut(peer, lr), piece(rp, row, col), s_row.at[d], r_row.at[d], {"row": peer})
        for d, peer in enumerate(row_peers)
    ]
    across = []
    for d, peer in enumerate(col_peers):
        for r in range(nr):
            part = piece(rp, r, col)
            across.append(
                remote(part, part, s_acr.at[d, r], r_acr.at[d, r], {"col": peer})
            )

    right, left = lax.rem(row + 1, nr), lax.rem(row + nr - 1, nr)
    groups = min(nc, 4)
    width = nc // groups

    def bundle(r, e):
        g = lax.rem(lax.div(col, width) - e + groups, groups)
        size = width * own
        return cp.at[pl.ds(pl.multiple_of((r * groups + g) * size, size), size)]

    def rightward(s, e):
        part = bundle(lax.rem(row - s + nr, nr), e)
        return remote(part, part, s_rt.at[s, e], r_rt.at[s, e], {"row": right})

    def leftward(s, e):
        part = bundle(lax.rem(row + s, nr), e)
        return remote(part, part, s_lt.at[s, e], r_lt.at[s, e], {"row": left})

    def sends(s):
        return (row >= s) & (row < nr - 1), (row + s < nr) & (row > 0)

    def start_chain(s, e):
        to_right, to_left = sends(s)

        @pl.when(to_right)
        def _():
            rightward(s, e).start()

        @pl.when(to_left)
        def _():
            leftward(s, e).start()

    def receive(s, e):
        @pl.when(row - 1 - s >= 0)
        def _():
            part = bundle(lax.rem(row - 1 - s + nr, nr), e)
            remote(part, part, s_rt.at[s, e], r_rt.at[s, e], {"row": right}).wait_recv()

        @pl.when(row + 1 + s < nr)
        def _():
            part = bundle(lax.rem(row + 1 + s, nr), e)
            remote(part, part, s_lt.at[s, e], r_lt.at[s, e], {"row": left}).wait_recv()

    def arrive(e):
        g = lax.rem(lax.div(col, width) - e + groups, groups)
        for w in range(width):
            back = lax.rem(col - (g * width + w) + nc, nc)

            @pl.when(back > 0)
            def _():
                d = lax.max(back - 1, 0)
                part = piece(cp, row, g * width + w)
                remote(part, part, s_col.at[d], r_col.at[d], {"col": col_peers[0]}).wait_recv()

    def absorb(i):
        def work():
            fetch(i).wait()
            tile[pl.ds(i * band, band), :] = stage[i % SLOTS].astype(BF16)
            if i + SLOTS < bands:
                fetch(i + SLOTS).start()

        return work

    keep_tile = pltpu.make_async_copy(tile, tile_out, out_sem.at[0])

    def begin(part):
        acc[:, part] = dot(vec[...], tile[:, part])

    chunk = min(512, lc)
    todo = [absorb(i) for i in range(bands)] + [keep_tile.start]
    todo += [functools.partial(begin, pl.ds(j * chunk, chunk)) for j in range(lc // chunk)]

    for s in range(nr - 1):
        for e in range(groups):
            if s == 0:
                arrive(e)
            else:
                receive(s - 1, e)
            start_chain(s, e)
            if s == 0 and e == groups - 1:
                for copy in by_row:
                    copy.start()
            if s == min(2, nr - 2) and e == groups - 1:
                for copy in by_row:
                    copy.wait_recv()
                for copy in across:
                    copy.start()
            if todo:
                todo.pop(0)()
    while todo:
        todo.pop(0)()
    for e in range(groups):
        receive(nr - 2, e)
    for copy in across:
        copy.wait_recv()
    keep_rp = pltpu.make_async_copy(rp, rp_out, out_sem.at[1])
    keep_cp = pltpu.make_async_copy(cp, cp_out, out_sem.at[2])
    keep_rp.start()
    keep_cp.start()

    started = []

    def row_sum(bufs, during=None):
        mine, theirs, chip, zbuf, total, land = bufs[:6]
        s_p, r_p, s_z, r_z, s_g, r_g, s_f, r_f = bufs[6:]
        length = mine.shape[3]
        for h in range(2):
            for j in range(nz):
                low = (h * nz + j) * length
                mine[h, j] = acc[:, low : low + length].astype(BF16)
        swap = remote(mine.at[1 - core], theirs, s_p.at[0], r_p.at[0], {"row": partner})
        swap.start()
        swap.wait_recv()
        scatter = []
        for d, peer in enumerate(z_peers):
            chip[d] = (mine[core, peer].astype(F32) + theirs[peer].astype(F32)).astype(BF16)
            scatter.append(
                remote(chip.at[d], zbuf.at[d], s_z.at[d], r_z.at[d], {"row": 2 * peer + core})
            )
            scatter[-1].start()
        result = mine[core, zed].astype(F32) + theirs[zed].astype(F32)
        if during is not None:
            during()
        for d, copy in enumerate(scatter):
            copy.wait_recv()
            result = result + zbuf[d].astype(F32)
        total[...] = result.astype(BF16)
        land[core, zed] = result.astype(BF16)
        spread_out, forward = [], []
        for d, peer in enumerate(z_peers):
            spread_out.append(
                remote(total, land.at[core, zed], s_g.at[d], r_g.at[d], {"row": 2 * peer + core})
            )
            spread_out[-1].start()
        forward.append(
            remote(total, land.at[core, zed], s_f.at[0], r_f.at[0], {"row": partner})
        )
        forward[-1].start()
        for d in range(nz - 1):
            source = lax.rem(zed - d - 1 + nz, nz)
            part = land.at[core, source]
            remote(part, part, s_g.at[d], r_g.at[d], {"row": partner}).wait_recv()
            forward.append(
                remote(part, part, s_f.at[d + 1], r_f.at[d + 1], {"row": partner})
            )
            forward[-1].start()
        for d in range(nz):
            part = land.at[1 - core, lax.rem(zed - d + nz, nz)]
            remote(part, part, s_f.at[d], r_f.at[d], {"row": partner}).wait_recv()
        for h in range(2):
            for j in range(nz):
                low = (h * nz + j) * length
                image[:, low : low + length] = land[h, j].astype(F32)
        started.extend([swap] + scatter + spread_out + forward)

    def gram_send(axis, value, bufs):
        slots, out, s_g, r_g = bufs
        me, peers = (row, row_peers) if axis == "row" else (col, col_peers)
        out[...] = value
        slots[me] = value
        copies = []
        for d, peer in enumerate(peers):
            copies.append(remote(out, slots.at[me], s_g.at[d], r_g.at[d], {axis: peer}))
            copies[-1].start()
        started.extend(copies)
        return copies

    def gram_take(copies, bufs):
        for copy in copies:
            copy.wait_recv()
        total = bufs[0][0]
        for j in range(1, bufs[0].shape[0]):
            total = total + bufs[0][j]
        return total

    def note(step, diag):
        spectrum[step : step + 1, :] = diag[:, :count]

    weight = (dot(vec[...], rp[...], ROWS) * scale).astype(BF16)

    def finish(part):
        acc[:, part] = acc[:, part] + dot(weight, cp[:, part])

    loop(lc, 512, finish)
    row_sum(sums_a)

    first = image[...].astype(BF16)
    copies = gram_send("col", dot(first, first, ROWS), grams[:4])
    weight = (dot(first, cp[...], ROWS) * scale).astype(BF16)

    def middle(part):
        value = dot(image[...].astype(BF16), tile[part, :], ROWS) + dot(weight, rp[:, part])
        cs_land[col, :, part] = value.astype(BF16)

    loop(lr, 256, middle)
    exchange = []
    for d, peer in enumerate(col_peers):
        exchange.append(
            remote(cs_land.at[col], cs_land.at[col], s_cs.at[d], r_cs.at[d], {"col": peer})
        )
        exchange[-1].start()
    started.extend(exchange)
    inverse, diag = cholesky_inverse(gram_take(copies, grams[:4]), count)
    note(0, diag)
    for copy in exchange:
        copy.wait_recv()

    def normalize(part):
        block = cs_land[0, :, part].astype(F32)
        for j in range(1, nc):
            block = block + cs_land[j, :, part].astype(F32)
        vec[:, part] = dot(inverse, block, precision=lax.Precision.HIGHEST).astype(BF16)

    loop(lr, 512, normalize)

    second = vec[...]
    copies = gram_send("row", dot(second, second, ROWS), grams[4:8])
    weight = (dot(second, rp[...], ROWS) * scale).astype(BF16)

    def final(part):
        acc[:, part] = dot(vec[...], tile[:, part]) + dot(weight, cp[:, part])

    loop(lc, 512, final)
    kept = []

    def factor_second():
        kept.extend(cholesky_inverse(gram_take(copies, grams[4:8]), count))

    row_sum(sums_b, factor_second)
    inverse, diag = kept
    note(1, diag)

    def settle(part):
        acc[:, part] = dot(inverse, image[:, part], precision=lax.Precision.HIGHEST)

    loop(lc, 512, settle)
    third = acc[...].astype(BF16)
    copies = gram_send("col", dot(third, third, ROWS), grams[8:12])
    inverse, diag = cholesky_inverse(gram_take(copies, grams[8:12]), count)
    note(2, diag)
    inverse = inverse * root

    def emit(part):
        value = dot(inverse, acc[:, part], precision=lax.Precision.HIGHEST)
        pcs[:, part] = value[:count]

    loop(lc, 512, emit)

    for copy in by_col + by_row + across + started:
        copy.wait_send()
    for s in range(nr - 1):
        to_right, to_left = sends(s)
        for e in range(groups):

            @pl.when(to_right)
            def _():
                rightward(s, e).wait_send()

            @pl.when(to_left)
            def _():
                leftward(s, e).wait_send()

    keep_tile.wait()
    keep_rp.wait()
    keep_cp.wait()


def main_call(genotypes, snp_index, freq_table, prior, start):
    nr, nc = lax.axis_size("row"), lax.axis_size("col")
    own, samples = genotypes.shape
    depth = own * nr * nc
    lr, lc = prior.shape
    count = start.shape[0]
    height = -(-count // 32) * 32
    groups = min(nc, 4)
    nz = nr // 2
    length = lc // nr
    dma = pltpu.SemaphoreType.DMA
    vmem = pl.BlockSpec(memory_space=pltpu.VMEM)
    smem = pl.BlockSpec(memory_space=pltpu.SMEM)
    hbm = pl.BlockSpec(memory_space=pl.ANY)
    band = min(128, lr)

    def sum_scratch():
        return [
            pltpu.VMEM((2, nz, height, length), BF16),
            pltpu.VMEM((nz, height, length), BF16),
            pltpu.VMEM((nz - 1, height, length), BF16),
            pltpu.VMEM((nz - 1, height, length), BF16),
            pltpu.VMEM((height, length), BF16),
            pltpu.VMEM((2, nz, height, length), BF16),
            dma((1,)),
            dma((1,)),
            dma((nz - 1,)),
            dma((nz - 1,)),
            dma((nz - 1,)),
            dma((nz - 1,)),
            dma((nz,)),
            dma((nz,)),
        ]

    def gram_scratch(n):
        return [
            pltpu.VMEM((n, height, height), F32),
            pltpu.VMEM((height, height), F32),
            dma((n - 1,)),
            dma((n - 1,)),
        ]

    scratch = [
        pltpu.VMEM((depth, lr), BF16),
        pltpu.VMEM((depth, lc), BF16),
        pltpu.VMEM((own, samples), BF16),
        pltpu.VMEM((lr, lc), BF16),
        pltpu.VMEM((SLOTS, band, lc), F32),
        pltpu.VMEM((height, lc), F32),
        pltpu.VMEM((height, lr), BF16),
        pltpu.VMEM((height, lc), F32),
        dma((SLOTS,)),
        dma((3,)),
        dma((nr - 1,)),
        dma((nr - 1,)),
        dma((nc - 1,)),
        dma((nc - 1,)),
        dma((nc - 1, nr)),
        dma((nc - 1, nr)),
    ]
    scratch += [dma((nr - 1, groups))] * 4
    scratch += sum_scratch() + sum_scratch()
    scratch += [pltpu.VMEM((nc, height, lr), BF16), dma((nc - 1,)), dma((nc - 1,))]
    scratch += gram_scratch(nc) + gram_scratch(nr) + gram_scratch(nc)
    return pl.pallas_call(
        functools.partial(main_kernel, nr, nc, count, float(samples) ** 0.5),
        in_specs=[smem, smem, vmem, vmem, hbm],
        out_specs=[hbm, hbm, hbm, vmem, vmem],
        out_shape=[
            jax.ShapeDtypeStruct((depth, lr), BF16),
            jax.ShapeDtypeStruct((depth, lc), BF16),
            jax.ShapeDtypeStruct((lr, lc), BF16),
            jax.ShapeDtypeStruct((count, lc), F32),
            jax.ShapeDtypeStruct((ITERS, count), F32),
        ],
        scratch_shapes=scratch,
        compiler_params=pltpu.CompilerParams(
            collective_id=20, has_side_effects=True, vmem_limit_bytes=60 * 2**20
        ),
        name="main",
    )(snp_index, freq_table, genotypes, start, prior)


def tile_kernel(scale, rows_ref, cols_ref, prior_ref, grm_ref):
    def part(cut):
        window = dot(rows_ref[...], cols_ref[:, cut], ((0,), (0,)))
        grm_ref[:, cut] = prior_ref[:, cut].astype(F32) + window * scale

    step = min(512, cols_ref.shape[1])
    for low in range(0, cols_ref.shape[1], step):
        part(slice(low, low + step))


def make_tile(row_panel, col_panel, prior):
    depth = row_panel.shape[0]
    rows, cols = prior.shape
    bm = min(256, rows)
    return pl.pallas_call(
        functools.partial(tile_kernel, 1.0 / depth),
        grid=(rows // bm,),
        in_specs=[
            pl.BlockSpec((depth, bm), lambda i: (0, i)),
            pl.BlockSpec((depth, cols), lambda i: (0, 0)),
            pl.BlockSpec((bm, cols), lambda i: (i, 0)),
        ],
        out_specs=pl.BlockSpec((bm, cols), lambda i: (i, 0)),
        out_shape=jax.ShapeDtypeStruct((rows, cols), F32),
        compiler_params=pltpu.CompilerParams(
            dimension_semantics=("arbitrary",), vmem_limit_bytes=56 * 2**20
        ),
        cost_estimate=pl.CostEstimate(
            flops=2 * rows * cols * depth, bytes_accessed=6 * rows * cols, transcendentals=0
        ),
        name="tile",
    )(row_panel, col_panel, prior)


def body(genotypes, snp_index, freq_table, prior, start_vectors):
    row_panel, col_panel, tile, pcs, spectrum = main_call(
        genotypes, snp_index, freq_table, prior, start_vectors.T
    )
    return make_tile(row_panel, col_panel, tile), pcs.T, spectrum


def solution(mesh):
    return jax.shard_map(
        body,
        mesh=mesh,
        in_specs=(P(("row", "col"), None), P(("row", "col")), P(), P("row", "col"), P("row", None)),
        out_specs=(P("row", "col"), P("col", None), P()),
        check_vma=False,
    )
```

```python
import functools

import jax
import jax.numpy as jnp
from jax import lax
from jax.experimental import pallas as pl
from jax.experimental.pallas import tpu as pltpu
from jax.sharding import PartitionSpec as P

ITERS = 3
MESH = pl.DeviceIdType.MESH
SLOTS = 4
HEIGHT = 8
F32, BF16 = jnp.float32, jnp.bfloat16


def dot(a, b, dims=((1,), (0,)), precision=None):
    return lax.dot_general(
        a, b, (dims, ((), ())), precision=precision, preferred_element_type=jnp.float32
    )


ROWS = ((1,), (1,))


def loop(size, step, body):
    step = min(step, size)

    def one(j, carry):
        body(pl.ds(pl.multiple_of(j * step, step), step))
        return carry

    lax.fori_loop(0, size // step, one, 0)


def swung(q, e):
    high, low = lax.div(q, 2) + e // 2, lax.rem(q, 2) + e % 2
    return 2 * lax.rem(high, 2) + lax.rem(low, 2)


def cholesky_inverse(gram, count):
    height = gram.shape[0]
    row = lax.broadcasted_iota(jnp.int32, (height, 128), 0)
    lane = lax.broadcasted_iota(jnp.int32, (height, 128), 1)
    eye = jnp.where(row == lane - height, 1.0, 0.0).astype(F32)
    both = jnp.concatenate([gram, jnp.zeros((height, 128 - height), F32)], axis=1) + eye
    diag = jnp.zeros((1, 128), F32)
    for k in range(count):
        pivot = both[k : k + 1, k : k + 1]
        inv = lax.rsqrt(pivot)
        head = both[k : k + 1, :] * inv
        below = jnp.where(row[:, :1] > k, both[:, k : k + 1] * inv, 0.0)
        both = jnp.where(row == k, head, both - below * head)
        diag = jnp.where(lane[:1, :] == k, pivot * inv, diag)
    return both[:, height : 2 * height], diag


def main_kernel(nr, nc, count, root, *refs):
    idx_hbm, freq_hbm, geno_hbm, start_hbm, prior, rp, cp, tile, pcs, spectrum = refs[:10]
    refs = refs[10:]
    idx, freq, start, geno = refs[:4]
    refs = refs[4:]
    std, stage, acc, vec, image, begun, shares = refs[:7]
    refs = (None,) + refs
    stage_sem, load_sem = refs[8:10]
    s_row, r_row, s_col, r_col, s_acr, r_acr, s_rt, r_rt, s_lt, r_lt = refs[10:20]
    sums_a, sums_b = refs[20:34], refs[34:48]
    cs_land, s_cs, r_cs, s_sh, r_sh, s_dir, r_dir, s_hub, r_hub, s_fan, r_fan = refs[48:59]
    grams = refs[59:]

    row, col = lax.axis_index("row"), lax.axis_index("col")
    own, samples = std.shape
    depth, lr = rp.shape
    lc = cp.shape[1]
    height = vec.shape[0]
    nz = nr // 2
    core, zed = lax.rem(row, 2), lax.div(row, 2)
    scale = 1.0 / depth
    row_peers = [lax.rem(row + d, nr) for d in range(1, nr)]
    col_peers = [swung(col, d) if nc == 4 else lax.rem(col + d, nc) for d in range(1, nc)]
    z_peers = [lax.rem(zed + d, nz) for d in range(1, nz)]
    partner = row + 1 - 2 * core

    loads = []
    for source, target in ((idx_hbm, idx), (freq_hbm, freq), (start_hbm, start), (geno_hbm, geno)):
        loads.append(pltpu.make_async_copy(source, target, load_sem.at[len(loads)]))
        loads[-1].start()
    barrier = pltpu.get_barrier_semaphore()
    for peer in row_peers:
        pl.semaphore_signal(barrier, inc=1, device_id={"row": peer}, device_id_type=MESH)
    for peer in col_peers:
        pl.semaphore_signal(barrier, inc=1, device_id={"col": peer}, device_id_type=MESH)

    def remote(src, dst, send_sem, recv_sem, target):
        return pltpu.make_async_remote_copy(
            src_ref=src,
            dst_ref=dst,
            send_sem=send_sem,
            recv_sem=recv_sem,
            device_id=target,
            device_id_type=MESH,
        )

    band = stage.shape[1]
    bands = lr // band

    ratio = lc // lr
    hub = lax.div(row, ratio)
    offset = pl.multiple_of(lax.rem(row, ratio) * lr, 128)
    relayed = nc <= 4

    def fetch(i):
        return pltpu.make_async_copy(
            prior.at[pl.ds(i * band, band)], stage.at[i % SLOTS], stage_sem.at[i % SLOTS]
        )

    for i in range(min(SLOTS, bands)):
        fetch(i).start()

    loads[0].wait()
    loads[1].wait()
    place = lax.broadcasted_iota(jnp.int32, (own, 1), 0)
    allele = jnp.zeros((own, 1), F32)
    for j in range(own):
        allele = jnp.where(place == j, freq[idx[j]], allele)
    doubled = 2.0 * allele
    spread = jnp.sqrt(doubled * (1.0 - allele))
    levels = [(float(g) - doubled) / spread for g in range(3)]

    def standardize(part):
        g = geno[:, part]
        value = jnp.where(g == 0, levels[0], jnp.where(g == 1, levels[1], levels[2]))
        std[:, part] = value.astype(BF16)

    loads[3].wait()
    loop(samples, 2048, standardize)
    loads[2].wait()
    vec[...] = jnp.concatenate(
        [start[...] * (1.0 / root), jnp.zeros((height - count, lr), F32)], axis=0
    ).astype(BF16)

    pl.semaphore_wait(barrier, nr + nc - 2)

    def cut(index, length):
        return std.at[:, pl.ds(pl.multiple_of(index * length, 128), length)]

    def piece(panel, r, q):
        return panel.at[pl.ds(pl.multiple_of((r * nc + q) * own, own), own)]

    by_col = [
        remote(cut(peer, lc), piece(cp, row, col), s_col.at[d], r_col.at[d], {"col": peer})
        for d, peer in enumerate(col_peers)
    ]
    for copy in by_col:
        copy.start()
    piece(cp, row, col)[...] = cut(col, lc)[...]
    piece(rp, row, col)[...] = cut(row, lr)[...]

    by_row, across, direct = [], [], []
    if relayed:
        for d, peer in enumerate(col_peers):
            direct.append(
                remote(cut(row, lr), piece(rp, row, col), s_dir.at[d], r_dir.at[d], {"col": peer})
            )
    else:
        for d, peer in enumerate(row_peers):
            by_row.append(
                remote(cut(peer, lr), piece(rp, row, col), s_row.at[d], r_row.at[d], {"row": peer})
            )
        for d, peer in enumerate(col_peers):
            for r in range(nr):
                part = piece(rp, r, col)
                across.append(
                    remote(part, part, s_acr.at[d, r], r_acr.at[d, r], {"col": peer})
                )

    @pl.when(col == hub)
    def _():
        begun[lax.rem(row, ratio)] = vec[...]

    right, left = lax.rem(row + 1, nr), lax.rem(row + nr - 1, nr)
    groups = min(nc, 4)
    width = nc // groups

    def group(base, e):
        mine = lax.div(base, width)
        return swung(mine, e) if groups == 4 else lax.rem(mine - e + groups, groups)

    def bundle(r, e, panel=None, base=None):
        base = col if base is None else base
        g = group(base, e)
        size = width * own
        part = pl.ds(pl.multiple_of((r * groups + g) * size, size), size)
        return (cp if panel is None else panel).at[part]

    def packet(r, e):
        return begun.at[lax.rem(r, ratio)] if e == groups else bundle(r, e)

    def wanted(r, e):
        return lax.div(r, ratio) == col if e == groups else True

    def rightward(s, e):
        part = packet(lax.rem(row - s + nr, nr), e)
        return remote(part, part, s_rt.at[s, e], r_rt.at[s, e], {"row": right})

    def leftward(s, e):
        part = packet(lax.rem(row + s, nr), e)
        return remote(part, part, s_lt.at[s, e], r_lt.at[s, e], {"row": left})

    def sends(s, e):
        to_right = (row >= s) & (row < nr - 1) & wanted(lax.rem(row - s + nr, nr), e)
        to_left = (row + s < nr) & (row > 0) & wanted(lax.rem(row + s, nr), e)
        return to_right, to_left

    def start_chain(s, e):
        to_right, to_left = sends(s, e)

        @pl.when(to_right)
        def _():
            rightward(s, e).start()

        @pl.when(to_left)
        def _():
            leftward(s, e).start()

    def receive(s, e):
        from_left = lax.rem(row - 1 - s + nr, nr)
        from_right = lax.rem(row + 1 + s, nr)

        @pl.when((row - 1 - s >= 0) & wanted(from_left, e))
        def _():
            part = packet(from_left, e)
            remote(part, part, s_rt.at[s, e], r_rt.at[s, e], {"row": right}).wait_recv()

        @pl.when((row + 1 + s < nr) & wanted(from_right, e))
        def _():
            part = packet(from_right, e)
            remote(part, part, s_lt.at[s, e], r_lt.at[s, e], {"row": left}).wait_recv()

    def hand(s, e, act):
        for way in range(2):
            k = (s * groups + e) * 2 + way
            r = lax.rem(row + 1 + s, nr) if way else lax.rem(row - 1 - s + nr, nr)
            valid = (row + 1 + s < nr) if way else (row - 1 - s >= 0)
            turn = k % (nc - 1)
            middle = lax.rem(hub + 1 + turn, nc)
            part = bundle(r, e, rp, hub)

            def feed():
                source = bundle(r, e).at[:, pl.ds(offset, lr)]
                return remote(
                    source, part, s_hub.at[s, e, way], r_hub.at[s, e, way], {"col": middle}
                )

            def fan(m):
                target = lax.rem(hub + 1 + (turn + m) % (nc - 1), nc)
                return remote(
                    part, part, s_fan.at[s, e, way, m - 1], r_fan.at[s, e, way], {"col": target}
                )

            if act == "feed":

                @pl.when(valid & (col == hub))
                def _():
                    feed().start()
                    part[...] = bundle(r, e)[:, pl.ds(offset, lr)]

            if act == "fan":

                @pl.when(valid & (col == middle))
                def _():
                    feed().wait_recv()
                    for m in range(1, nc - 1):
                        fan(m).start()

            if act == "land":

                @pl.when(valid & (col != hub) & (col != middle))
                def _():
                    fan(1).wait_recv()

            if act == "drain":

                @pl.when(valid & (col == hub))
                def _():
                    feed().wait_send()

                @pl.when(valid & (col == middle))
                def _():
                    for m in range(1, nc - 1):
                        fan(m).wait_send()

    def hand_all(act):
        if relayed:
            for s in range(nr - 1):
                for e in range(groups):
                    hand(s, e, act)

    def arrive(e):
        g = group(col, e)
        if nc == 4:
            if e > 0:
                part = piece(cp, row, g)
                remote(
                    part, part, s_col.at[e - 1], r_col.at[e - 1], {"col": col_peers[0]}
                ).wait_recv()
            return
        for w in range(width):
            back = lax.rem(col - (g * width + w) + nc, nc)

            @pl.when(back > 0)
            def _():
                d = lax.max(back - 1, 0)
                part = piece(cp, row, g * width + w)
                remote(part, part, s_col.at[d], r_col.at[d], {"col": col_peers[0]}).wait_recv()

    def absorb(i):
        def work():
            fetch(i).wait()
            tile[pl.ds(i * band, band), :] = stage[i % SLOTS].astype(BF16)
            if i + SLOTS < bands:
                fetch(i + SLOTS).start()

        return work

    started = []

    def row_sum(bufs, during=None):
        mine, theirs, chip, zbuf, total, land = bufs[:6]
        s_p, r_p, s_z, r_z, s_g, r_g, s_f, r_f = bufs[6:]
        length = mine.shape[3]
        for h in range(2):
            for j in range(nz):
                low = (h * nz + j) * length
                mine[h, j] = acc[:, low : low + length].astype(BF16)
        swap = remote(mine.at[1 - core], theirs, s_p.at[0], r_p.at[0], {"row": partner})
        swap.start()
        yield
        swap.wait_recv()
        scatter = []
        for d, peer in enumerate(z_peers):
            chip[d] = (mine[core, peer].astype(F32) + theirs[peer].astype(F32)).astype(BF16)
            scatter.append(
                remote(chip.at[d], zbuf.at[d], s_z.at[d], r_z.at[d], {"row": 2 * peer + core})
            )
            scatter[-1].start()
        result = mine[core, zed].astype(F32) + theirs[zed].astype(F32)
        if during is not None:
            during()
        yield
        for d, copy in enumerate(scatter):
            copy.wait_recv()
            result = result + zbuf[d].astype(F32)
        total[...] = result.astype(BF16)
        land[core, zed] = result.astype(BF16)
        spread_out, forward = [], []
        for d, peer in enumerate(z_peers):
            spread_out.append(
                remote(total, land.at[core, zed], s_g.at[d], r_g.at[d], {"row": 2 * peer + core})
            )
            spread_out[-1].start()
        forward.append(
            remote(total, land.at[core, zed], s_f.at[0], r_f.at[0], {"row": partner})
        )
        forward[-1].start()
        yield
        for d in range(nz - 1):
            source = lax.rem(zed - d - 1 + nz, nz)
            part = land.at[core, source]
            remote(part, part, s_g.at[d], r_g.at[d], {"row": partner}).wait_recv()
            forward.append(
                remote(part, part, s_f.at[d + 1], r_f.at[d + 1], {"row": partner})
            )
            forward[-1].start()
        yield
        for d in range(nz):
            part = land.at[1 - core, lax.rem(zed - d + nz, nz)]
            remote(part, part, s_f.at[d], r_f.at[d], {"row": partner}).wait_recv()
        for h in range(2):
            for j in range(nz):
                low = (h * nz + j) * length
                image[:, low : low + length] = land[h, j].astype(F32)
        started.extend([swap] + scatter + spread_out + forward)

    def begin(part):
        acc[:, part] = dot(vec[...], tile[:, part])

    chunk = min(512, lc)
    todo = [absorb(i) for i in range(bands)]
    todo += [functools.partial(begin, pl.ds(j * chunk, chunk)) for j in range(lc // chunk)]
    todo = [todo[i : i + 2] for i in range(0, len(todo), 2)]
    stages = row_sum(sums_a)
    step_on = [lambda: next(stages, None)]
    for gap in (1, 6, 6):
        todo += [step_on] + [[]] * gap

    for s in range(nr - 1):
        for e in range(groups):
            if s == 0:
                arrive(e)
            else:
                receive(s - 1, e)
            start_chain(s, e)
            if relayed and s > 0:
                hand(s - 1, e, "feed")
            if relayed and s > 1:
                hand(s - 2, e, "fan")
            if todo:
                for work in todo.pop(0):
                    work()
        if s > 0:
            receive(s - 1, groups)
        start_chain(s, groups)
        if s == 0:
            for copy in by_row + direct:
                copy.start()
        if s == min(2, nr - 2):
            for copy in by_row:
                copy.wait_recv()
            for copy in across:
                copy.start()
    for e in range(groups + 1):
        receive(nr - 2, e)
        if relayed and e < groups:
            hand(nr - 2, e, "feed")
            hand(nr - 3, e, "fan")
    while todo:
        for work in todo.pop(0):
            work()

    for i in range(ratio):
        part = dot(begun[i], cp[:, i * lr : (i + 1) * lr], ROWS)
        share = part if i == 0 else share + part
    shares[col] = share.astype(BF16)
    swaps = []
    for d, peer in enumerate(col_peers):
        swaps.append(
            remote(shares.at[col], shares.at[col], s_sh.at[d], r_sh.at[d], {"col": peer})
        )
        swaps[-1].start()
    started.extend(swaps)
    if relayed:
        for e in range(groups):
            hand(nr - 2, e, "fan")
    for _ in stages:
        pass
    for copy in swaps:
        copy.wait_recv()
    share = shares[0].astype(F32)
    for j in range(1, nc):
        share = share + shares[j].astype(F32)
    weight = (share * scale).astype(BF16)

    def complete(part):
        image[:, part] = image[:, part] + dot(weight, cp[:, part])

    loop(lc, 512, complete)

    def gram_send(axis, value, bufs):
        slots, out, s_g, r_g = bufs
        me, peers = (row, row_peers) if axis == "row" else (col, col_peers)
        out[...] = value
        slots[me] = value
        copies = []
        for d, peer in enumerate(peers):
            copies.append(remote(out, slots.at[me], s_g.at[d], r_g.at[d], {axis: peer}))
            copies[-1].start()
        started.extend(copies)
        return copies

    def gram_take(copies, bufs):
        for copy in copies:
            copy.wait_recv()
        total = bufs[0][0]
        for j in range(1, bufs[0].shape[0]):
            total = total + bufs[0][j]
        return total

    def note(step, diag):
        spectrum[step : step + 1, :] = diag[:, :count]

    first = image[...].astype(BF16)
    copies = gram_send("col", dot(first, first, ROWS), grams[:4])
    weight = (dot(first, cp[...], ROWS) * scale).astype(BF16)

    parts = nc if lr % (128 * nc) == 0 else 1
    span = lr // parts
    exchange = []

    def middle(part):
        acc[:, part] = dot(first, tile[part, :], ROWS)

    loop(lr, 256, middle)
    hand_all("land")
    for copy in direct + across:
        copy.wait_recv()

    for p in range(parts):
        low = p * span
        value = acc[:, low : low + span] + dot(weight, rp[:, low : low + span])
        cs_land[p, col] = value.astype(BF16)
        for d, peer in enumerate(col_peers):
            mine = cs_land.at[p, col]
            exchange.append(remote(mine, mine, s_cs.at[d, p], r_cs.at[d, p], {"col": peer}))
            exchange[-1].start()
    started.extend(exchange)
    inverse, diag = cholesky_inverse(gram_take(copies, grams[:4]), count)
    note(0, diag)
    for p in range(parts):
        for copy in exchange[p * (nc - 1) : (p + 1) * (nc - 1)]:
            copy.wait_recv()
        block = cs_land[p, 0].astype(F32)
        for j in range(1, nc):
            block = block + cs_land[p, j].astype(F32)
        value = dot(inverse, block, precision=lax.Precision.HIGHEST)
        vec[:, p * span : (p + 1) * span] = value.astype(BF16)

    second = vec[...]
    copies = gram_send("row", dot(second, second, ROWS), grams[4:8])
    weight = (dot(second, rp[...], ROWS) * scale).astype(BF16)

    def final(part):
        acc[:, part] = dot(vec[...], tile[:, part]) + dot(weight, cp[:, part])

    loop(lc, 512, final)
    kept = []

    def factor_second():
        kept.extend(cholesky_inverse(gram_take(copies, grams[4:8]), count))

    for _ in row_sum(sums_b, factor_second):
        pass
    inverse, diag = kept
    note(1, diag)

    def settle(part):
        acc[:, part] = dot(inverse, image[:, part], precision=lax.Precision.HIGHEST)

    loop(lc, 512, settle)
    third = acc[...].astype(BF16)
    copies = gram_send("col", dot(third, third, ROWS), grams[8:12])
    inverse, diag = cholesky_inverse(gram_take(copies, grams[8:12]), count)
    note(2, diag)
    inverse = inverse * root

    def emit(part):
        value = dot(inverse, acc[:, part], precision=lax.Precision.HIGHEST)
        pcs[:, part] = value[:count]

    loop(lc, 512, emit)

    for copy in by_col + by_row + across + direct + started:
        copy.wait_send()
    for s in range(nr - 1):
        for e in range(groups + 1):
            to_right, to_left = sends(s, e)

            @pl.when(to_right)
            def _():
                rightward(s, e).wait_send()

            @pl.when(to_left)
            def _():
                leftward(s, e).wait_send()

    hand_all("drain")


def main_call(genotypes, snp_index, freq_table, prior, start):
    nr, nc = lax.axis_size("row"), lax.axis_size("col")
    own, samples = genotypes.shape
    depth = own * nr * nc
    lr, lc = prior.shape
    count = start.shape[0]
    height = -(-count // HEIGHT) * HEIGHT
    groups = min(nc, 4)
    nz = nr // 2
    length = lc // nr
    dma = pltpu.SemaphoreType.DMA
    vmem = pl.BlockSpec(memory_space=pltpu.VMEM)
    hbm = pl.BlockSpec(memory_space=pltpu.HBM)
    band = min(128, lr)

    def sum_scratch():
        return [
            pltpu.VMEM((2, nz, height, length), BF16),
            pltpu.VMEM((nz, height, length), BF16),
            pltpu.VMEM((nz - 1, height, length), BF16),
            pltpu.VMEM((nz - 1, height, length), BF16),
            pltpu.VMEM((height, length), BF16),
            pltpu.VMEM((2, nz, height, length), BF16),
            dma((1,)),
            dma((1,)),
            dma((nz - 1,)),
            dma((nz - 1,)),
            dma((nz - 1,)),
            dma((nz - 1,)),
            dma((nz,)),
            dma((nz,)),
        ]

    def gram_scratch(n):
        return [
            pltpu.VMEM((n, height, height), F32),
            pltpu.VMEM((height, height), F32),
            dma((n - 1,)),
            dma((n - 1,)),
        ]

    one = nr - 1 if nc <= 4 else 1
    scratch = [
        pltpu.SMEM((own,), jnp.int32),
        pltpu.SMEM(freq_table.shape, F32),
        pltpu.VMEM((count, lr), F32),
        pltpu.VMEM((own, samples), jnp.int32),
        pltpu.VMEM((own, samples), BF16),
        pltpu.VMEM((SLOTS, band, lc), F32),
        pltpu.VMEM((height, lc), F32),
        pltpu.VMEM((height, lr), BF16),
        pltpu.VMEM((height, lc), F32),
        pltpu.VMEM((lc // lr, height, lr), BF16),
        pltpu.VMEM((nc, height, depth), BF16),
        dma((SLOTS,)),
        dma((4,)),
        dma((nr - 1,)),
        dma((nr - 1,)),
        dma((nc - 1,)),
        dma((nc - 1,)),
        dma((nc - 1, nr)),
        dma((nc - 1, nr)),
    ]
    scratch += [dma((nr - 1, groups + 1))] * 4
    scratch += sum_scratch() + sum_scratch()
    parts = nc if lr % (128 * nc) == 0 else 1
    scratch += [pltpu.VMEM((parts, nc, height, lr // parts), BF16)]
    scratch += [dma((nc - 1, parts))] * 2
    scratch += [dma((nc - 1,))] * 4
    scratch += [dma((one, groups, 2))] * 2 + [dma((one, groups, 2, nc - 2)), dma((one, groups, 2))]
    scratch += gram_scratch(nc) + gram_scratch(nr) + gram_scratch(nc)
    args = (snp_index, freq_table, genotypes, start, prior)
    return pl.pallas_call(
        functools.partial(main_kernel, nr, nc, count, float(samples) ** 0.5),
        in_specs=[hbm] * 5,
        out_specs=[vmem] * 5,
        out_shape=[
            jax.ShapeDtypeStruct((depth, lr), BF16),
            jax.ShapeDtypeStruct((depth, lc), BF16),
            jax.ShapeDtypeStruct((lr, lc), BF16),
            jax.ShapeDtypeStruct((count, lc), F32),
            jax.ShapeDtypeStruct((ITERS, count), F32),
        ],
        scratch_shapes=scratch,
        compiler_params=pltpu.CompilerParams(
            collective_id=20, has_side_effects=True, vmem_limit_bytes=22 * 2**20
        ),
        name="main",
    )(*[pltpu.with_memory_space_constraint(x, pltpu.HBM) for x in args])


def tile_kernel(scale, rows_ref, cols_ref, prior_ref, pcs_ref, spectrum_ref, grm_ref, v_ref, d_ref):
    @pl.when(pl.program_id(0) == 0)
    def _():
        v_ref[...] = pcs_ref[...]
        d_ref[...] = spectrum_ref[...]

    def part(cut):
        window = dot(rows_ref[...], cols_ref[:, cut], ((0,), (0,)))
        grm_ref[:, cut] = prior_ref[:, cut].astype(F32) + window * scale

    step = min(512, cols_ref.shape[1])
    for low in range(0, cols_ref.shape[1], step):
        part(slice(low, low + step))


def make_tile(row_panel, col_panel, prior, pcs, spectrum):
    depth = row_panel.shape[0]
    rows, cols = prior.shape
    bm = min(256, rows)
    return pl.pallas_call(
        functools.partial(tile_kernel, 1.0 / depth),
        grid=(rows // bm,),
        in_specs=[
            pl.BlockSpec((depth, bm), lambda i: (0, i)),
            pl.BlockSpec((depth, cols), lambda i: (0, 0)),
            pl.BlockSpec((bm, cols), lambda i: (i, 0)),
            pl.BlockSpec(pcs.shape, lambda i: (0, 0)),
            pl.BlockSpec(spectrum.shape, lambda i: (0, 0)),
        ],
        out_specs=[
            pl.BlockSpec((bm, cols), lambda i: (i, 0)),
            pl.BlockSpec(pcs.shape, lambda i: (0, 0)),
            pl.BlockSpec(spectrum.shape, lambda i: (0, 0)),
        ],
        out_shape=[
            jax.ShapeDtypeStruct((rows, cols), F32),
            jax.ShapeDtypeStruct(pcs.shape, F32),
            jax.ShapeDtypeStruct(spectrum.shape, F32),
        ],
        compiler_params=pltpu.CompilerParams(
            dimension_semantics=("arbitrary",), vmem_limit_bytes=24 * 2**20
        ),
        cost_estimate=pl.CostEstimate(
            flops=2 * rows * cols * depth, bytes_accessed=6 * rows * cols, transcendentals=0
        ),
        name="tile",
    )(row_panel, col_panel, prior, pcs, spectrum)


def body(genotypes, snp_index, freq_table, prior, start_vectors):
    row_panel, col_panel, tile, pcs, spectrum = main_call(
        genotypes, snp_index, freq_table, prior, start_vectors.T
    )
    grm, pcs, spectrum = make_tile(row_panel, col_panel, tile, pcs, spectrum)
    return grm, pcs.T, spectrum


def solution(mesh):
    return jax.shard_map(
        body,
        mesh=mesh,
        in_specs=(P(("row", "col"), None), P(("row", "col")), P(), P("row", "col"), P("row", None)),
        out_specs=(P("row", "col"), P("col", None), P()),
        check_vma=False,
    )
```

```python
import functools

import jax
import jax.numpy as jnp
from jax import lax
from jax.experimental import pallas as pl
from jax.experimental.pallas import tpu as pltpu
from jax.sharding import PartitionSpec as P

ITERS = 3
MESH = pl.DeviceIdType.MESH
SLOTS = 4
HEIGHT = 8
LAG = 2
F32, BF16 = jnp.float32, jnp.bfloat16


def dot(a, b, dims=((1,), (0,)), precision=None):
    return lax.dot_general(
        a, b, (dims, ((), ())), precision=precision, preferred_element_type=jnp.float32
    )


ROWS = ((1,), (1,))


def loop(size, step, body):
    step = min(step, size)

    def one(j, carry):
        body(pl.ds(pl.multiple_of(j * step, step), step))
        return carry

    lax.fori_loop(0, size // step, one, 0)


def swung(q, e):
    high, low = lax.div(q, 2) + e // 2, lax.rem(q, 2) + e % 2
    return 2 * lax.rem(high, 2) + lax.rem(low, 2)


def cholesky_inverse(gram, count):
    height = gram.shape[0]
    row = lax.broadcasted_iota(jnp.int32, (height, 128), 0)
    lane = lax.broadcasted_iota(jnp.int32, (height, 128), 1)
    eye = jnp.where(row == lane - height, 1.0, 0.0).astype(F32)
    both = jnp.concatenate([gram, jnp.zeros((height, 128 - height), F32)], axis=1) + eye
    diag = jnp.zeros((1, 128), F32)
    for k in range(count):
        pivot = both[k : k + 1, k : k + 1]
        inv = lax.rsqrt(pivot)
        head = both[k : k + 1, :] * inv
        below = jnp.where(row[:, :1] > k, both[:, k : k + 1] * inv, 0.0)
        both = jnp.where(row == k, head, both - below * head)
        diag = jnp.where(lane[:1, :] == k, pivot * inv, diag)
    return both[:, height : 2 * height], diag


def main_kernel(nr, nc, count, root, *refs):
    idx_hbm, freq_hbm, geno_hbm, start_hbm, prior, rp, cp, tile, pcs, spectrum = refs[:10]
    refs = refs[10:]
    idx, freq, start, geno = refs[:4]
    refs = refs[4:]
    std, stage, acc, vec, image, begun, shares = refs[:7]
    refs = (None,) + refs
    stage_sem, load_sem = refs[8:10]
    s_row, r_row, s_col, r_col, s_acr, r_acr, s_rt, r_rt, s_lt, r_lt = refs[10:20]
    sums_a, sums_b = refs[20:34], refs[34:48]
    cs_land, s_cs, r_cs, s_sh, r_sh, s_dir, r_dir, s_hub, r_hub, s_fan, r_fan = refs[48:59]
    grams = refs[59:]

    row, col = lax.axis_index("row"), lax.axis_index("col")
    own, samples = std.shape
    depth, lr = rp.shape
    lc = cp.shape[1]
    height = vec.shape[0]
    nz = nr // 2
    core, zed = lax.rem(row, 2), lax.div(row, 2)
    scale = 1.0 / depth
    row_peers = [lax.rem(row + d, nr) for d in range(1, nr)]
    col_peers = [swung(col, d) if nc == 4 else lax.rem(col + d, nc) for d in range(1, nc)]
    z_peers = [lax.rem(zed + d, nz) for d in range(1, nz)]
    partner = row + 1 - 2 * core

    loads = []
    for source, target in ((idx_hbm, idx), (freq_hbm, freq), (start_hbm, start), (geno_hbm, geno)):
        loads.append(pltpu.make_async_copy(source, target, load_sem.at[len(loads)]))
        loads[-1].start()
    barrier = pltpu.get_barrier_semaphore()
    for peer in row_peers:
        pl.semaphore_signal(barrier, inc=1, device_id={"row": peer}, device_id_type=MESH)
    for peer in col_peers:
        pl.semaphore_signal(barrier, inc=1, device_id={"col": peer}, device_id_type=MESH)

    def remote(src, dst, send_sem, recv_sem, target):
        return pltpu.make_async_remote_copy(
            src_ref=src,
            dst_ref=dst,
            send_sem=send_sem,
            recv_sem=recv_sem,
            device_id=target,
            device_id_type=MESH,
        )

    band = stage.shape[1]
    bands = lr // band

    ratio = lc // lr
    hub = lax.div(row, ratio)
    offset = pl.multiple_of(lax.rem(row, ratio) * lr, 128)
    relayed = nc <= 4

    def fetch(i):
        return pltpu.make_async_copy(
            prior.at[pl.ds(i * band, band)], stage.at[i % SLOTS], stage_sem.at[i % SLOTS]
        )

    for i in range(min(SLOTS, bands)):
        fetch(i).start()

    loads[0].wait()
    loads[1].wait()
    place = lax.broadcasted_iota(jnp.int32, (own, 1), 0)
    allele = jnp.zeros((own, 1), F32)
    for j in range(own):
        allele = jnp.where(place == j, freq[idx[j]], allele)
    doubled = 2.0 * allele
    spread = jnp.sqrt(doubled * (1.0 - allele))
    levels = [(float(g) - doubled) / spread for g in range(3)]

    def standardize(part):
        g = geno[:, part]
        value = jnp.where(g == 0, levels[0], jnp.where(g == 1, levels[1], levels[2]))
        std[:, part] = value.astype(BF16)

    loads[3].wait()
    loop(samples, 2048, standardize)
    loads[2].wait()
    vec[...] = jnp.concatenate(
        [start[...] * (1.0 / root), jnp.zeros((height - count, lr), F32)], axis=0
    ).astype(BF16)

    pl.semaphore_wait(barrier, nr + nc - 2)

    def cut(index, length):
        return std.at[:, pl.ds(pl.multiple_of(index * length, 128), length)]

    def piece(panel, r, q):
        return panel.at[pl.ds(pl.multiple_of((r * nc + q) * own, own), own)]

    by_col = [
        remote(cut(peer, lc), piece(cp, row, col), s_col.at[d], r_col.at[d], {"col": peer})
        for d, peer in enumerate(col_peers)
    ]
    for copy in by_col:
        copy.start()
    piece(cp, row, col)[...] = cut(col, lc)[...]
    piece(rp, row, col)[...] = cut(row, lr)[...]

    by_row, across, direct = [], [], []
    if relayed:
        for d, peer in enumerate(col_peers):
            direct.append(
                remote(cut(row, lr), piece(rp, row, col), s_dir.at[d], r_dir.at[d], {"col": peer})
            )
    else:
        for d, peer in enumerate(row_peers):
            by_row.append(
                remote(cut(peer, lr), piece(rp, row, col), s_row.at[d], r_row.at[d], {"row": peer})
            )
        for d, peer in enumerate(col_peers):
            for r in range(nr):
                part = piece(rp, r, col)
                across.append(
                    remote(part, part, s_acr.at[d, r], r_acr.at[d, r], {"col": peer})
                )

    @pl.when(col == hub)
    def _():
        begun[lax.rem(row, ratio)] = vec[...]

    right, left = lax.rem(row + 1, nr), lax.rem(row + nr - 1, nr)
    groups = min(nc, 4)
    width = nc // groups

    def group(base, e):
        mine = lax.div(base, width)
        return swung(mine, e) if groups == 4 else lax.rem(mine - e + groups, groups)

    def bundle(r, e, panel=None, base=None):
        base = col if base is None else base
        g = group(base, e)
        size = width * own
        part = pl.ds(pl.multiple_of((r * groups + g) * size, size), size)
        return (cp if panel is None else panel).at[part]

    def packet(r, e):
        return begun.at[lax.rem(r, ratio)] if e == groups else bundle(r, e)

    def wanted(r, e):
        return lax.div(r, ratio) == col if e == groups else True

    def rightward(s, e):
        part = packet(lax.rem(row - s + nr, nr), e)
        return remote(part, part, s_rt.at[s, e], r_rt.at[s, e], {"row": right})

    def leftward(s, e):
        part = packet(lax.rem(row + s, nr), e)
        return remote(part, part, s_lt.at[s, e], r_lt.at[s, e], {"row": left})

    def sends(s, e):
        to_right = (row >= s) & (row < nr - 1) & wanted(lax.rem(row - s + nr, nr), e)
        to_left = (row + s < nr) & (row > 0) & wanted(lax.rem(row + s, nr), e)
        return to_right, to_left

    def start_chain(s, e):
        to_right, to_left = sends(s, e)

        @pl.when(to_right)
        def _():
            rightward(s, e).start()

        @pl.when(to_left)
        def _():
            leftward(s, e).start()

    def receive(s, e):
        from_left = lax.rem(row - 1 - s + nr, nr)
        from_right = lax.rem(row + 1 + s, nr)

        @pl.when((row - 1 - s >= 0) & wanted(from_left, e))
        def _():
            part = packet(from_left, e)
            remote(part, part, s_rt.at[s, e], r_rt.at[s, e], {"row": right}).wait_recv()

        @pl.when((row + 1 + s < nr) & wanted(from_right, e))
        def _():
            part = packet(from_right, e)
            remote(part, part, s_lt.at[s, e], r_lt.at[s, e], {"row": left}).wait_recv()

    def hand(s, e, act):
        for way in range(2):
            k = (s * groups + e) * 2 + way
            r = lax.rem(row + 1 + s, nr) if way else lax.rem(row - 1 - s + nr, nr)
            valid = (row + 1 + s < nr) if way else (row - 1 - s >= 0)
            turn = k % (nc - 1)
            middle = lax.rem(hub + 1 + turn, nc)
            part = bundle(r, e, rp, hub)

            def feed():
                source = bundle(r, e).at[:, pl.ds(offset, lr)]
                return remote(
                    source, part, s_hub.at[s, e, way], r_hub.at[s, e, way], {"col": middle}
                )

            def fan(m):
                target = lax.rem(hub + 1 + (turn + m) % (nc - 1), nc)
                return remote(
                    part, part, s_fan.at[s, e, way, m - 1], r_fan.at[s, e, way], {"col": target}
                )

            if act == "feed":

                @pl.when(valid & (col == hub))
                def _():
                    feed().start()
                    part[...] = bundle(r, e)[:, pl.ds(offset, lr)]

            if act == "fan":

                @pl.when(valid & (col == middle))
                def _():
                    feed().wait_recv()
                    for m in range(1, nc - 1):
                        fan(m).start()

            if act == "land":

                @pl.when(valid & (col != hub) & (col != middle))
                def _():
                    fan(1).wait_recv()

            if act == "drain":

                @pl.when(valid & (col == hub))
                def _():
                    feed().wait_send()

                @pl.when(valid & (col == middle))
                def _():
                    for m in range(1, nc - 1):
                        fan(m).wait_send()

    def hand_all(act):
        if relayed:
            for s in range(nr - 1):
                for e in range(groups):
                    hand(s, e, act)

    def arrive(e):
        g = group(col, e)
        if nc == 4:
            if e > 0:
                part = piece(cp, row, g)
                remote(
                    part, part, s_col.at[e - 1], r_col.at[e - 1], {"col": col_peers[0]}
                ).wait_recv()
            return
        for w in range(width):
            back = lax.rem(col - (g * width + w) + nc, nc)

            @pl.when(back > 0)
            def _():
                d = lax.max(back - 1, 0)
                part = piece(cp, row, g * width + w)
                remote(part, part, s_col.at[d], r_col.at[d], {"col": col_peers[0]}).wait_recv()

    def absorb(i):
        def work():
            fetch(i).wait()
            tile[pl.ds(i * band, band), :] = stage[i % SLOTS].astype(BF16)
            if i + SLOTS < bands:
                fetch(i + SLOTS).start()

        return work

    started = []

    def row_sum(bufs, during=None, make=None):
        mine, theirs, chip, zbuf, total, land = bufs[:6]
        s_p, r_p, s_z, r_z, s_g, r_g, s_f, r_f = bufs[6:]
        length = mine.shape[3]
        swaps, scatter = [], []
        if make is None:
            for h in range(2):
                for j in range(nz):
                    low = (h * nz + j) * length
                    mine[h, j] = acc[:, low : low + length].astype(BF16)
            swaps.append(remote(mine.at[1 - core], theirs, s_p.at[0], r_p.at[0], {"row": partner}))
            swaps[0].start()
            yield
            swaps[0].wait_recv()
        else:
            for t, z in enumerate(z_peers + [zed]):
                mine[1 - core, z] = make((1 - core) * nz + z).astype(BF16)
                swaps.append(
                    remote(
                        mine.at[1 - core, z],
                        theirs.at[z],
                        s_p.at[t],
                        r_p.at[t],
                        {"row": partner},
                    )
                )
                swaps[-1].start()
        for t, z in enumerate(z_peers + [zed]):
            if make is None:
                result = mine[core, z].astype(F32)
            else:
                result = make(core * nz + z)
                swaps[t].wait_recv()
            result = result + theirs[z].astype(F32)
            if t < nz - 1:
                chip[t] = result.astype(BF16)
                scatter.append(
                    remote(chip.at[t], zbuf.at[t], s_z.at[t], r_z.at[t], {"row": 2 * z + core})
                )
                scatter[-1].start()
        if during is not None:
            during()
        yield
        for d, copy in enumerate(scatter):
            copy.wait_recv()
            result = result + zbuf[d].astype(F32)
        total[...] = result.astype(BF16)
        land[core, zed] = result.astype(BF16)
        spread_out, forward = [], []
        for d, peer in enumerate(z_peers):
            spread_out.append(
                remote(total, land.at[core, zed], s_g.at[d], r_g.at[d], {"row": 2 * peer + core})
            )
            spread_out[-1].start()
        forward.append(
            remote(total, land.at[core, zed], s_f.at[0], r_f.at[0], {"row": partner})
        )
        forward[-1].start()
        yield
        for d in range(nz - 1):
            source = lax.rem(zed - d - 1 + nz, nz)
            part = land.at[core, source]
            remote(part, part, s_g.at[d], r_g.at[d], {"row": partner}).wait_recv()
            forward.append(
                remote(part, part, s_f.at[d + 1], r_f.at[d + 1], {"row": partner})
            )
            forward[-1].start()
        yield
        for d in range(nz):
            part = land.at[1 - core, lax.rem(zed - d + nz, nz)]
            remote(part, part, s_f.at[d], r_f.at[d], {"row": partner}).wait_recv()
        if during is None:
            for h in range(2):
                for j in range(nz):
                    low = (h * nz + j) * length
                    image[:, low : low + length] = land[h, j].astype(F32)
        started.extend(swaps + scatter + spread_out + forward)

    def begin(part):
        acc[:, part] = dot(vec[...], tile[:, part])

    chunk = min(512, lc)
    todo = [absorb(i) for i in range(bands)]
    todo += [functools.partial(begin, pl.ds(j * chunk, chunk)) for j in range(lc // chunk)]
    todo = [todo[i : i + 2] for i in range(0, len(todo), 2)]
    stages = row_sum(sums_a)
    step_on = [lambda: next(stages, None)]
    for gap in (1, 4, 5):
        todo += [step_on] + [[]] * gap

    for s in range(nr - 1):
        for e in range(groups):
            if s == 0:
                arrive(e)
            else:
                receive(s - 1, e)
            start_chain(s, e)
            if relayed and s > 0:
                hand(s - 1, e, "feed")
            if relayed and s >= LAG:
                hand(s - LAG, e, "fan")
            if todo:
                for work in todo.pop(0):
                    work()
        if s > 0:
            receive(s - 1, groups)
        start_chain(s, groups)
        if s == 0:
            for copy in by_row + direct:
                copy.start()
        if s == min(2, nr - 2):
            for copy in by_row:
                copy.wait_recv()
            for copy in across:
                copy.start()
    for e in range(groups + 1):
        receive(nr - 2, e)
        if relayed and e < groups:
            hand(nr - 2, e, "feed")
            for q in range(max(nr - 1 - LAG, 0), nr - 2):
                hand(q, e, "fan")
    while todo:
        for work in todo.pop(0):
            work()

    for i in range(ratio):
        part = dot(begun[i], cp[:, i * lr : (i + 1) * lr], ROWS)
        share = part if i == 0 else share + part
    shares[col] = share.astype(BF16)
    swaps = []
    for d, peer in enumerate(col_peers):
        swaps.append(
            remote(shares.at[col], shares.at[col], s_sh.at[d], r_sh.at[d], {"col": peer})
        )
        swaps[-1].start()
    started.extend(swaps)
    if relayed:
        for e in range(groups):
            hand(nr - 2, e, "fan")
    for _ in stages:
        pass
    for copy in swaps:
        copy.wait_recv()
    share = shares[0].astype(F32)
    for j in range(1, nc):
        share = share + shares[j].astype(F32)
    weight = (share * scale).astype(BF16)

    def complete(part):
        image[:, part] = image[:, part] + dot(weight, cp[:, part])

    loop(lc, 512, complete)

    def gram_send(axis, value, bufs):
        slots, out, s_g, r_g = bufs
        me, peers = (row, row_peers) if axis == "row" else (col, col_peers)
        out[...] = value
        slots[me] = value
        copies = []
        for d, peer in enumerate(peers):
            copies.append(remote(out, slots.at[me], s_g.at[d], r_g.at[d], {axis: peer}))
            copies[-1].start()
        started.extend(copies)
        return copies

    def gram_take(copies, bufs):
        for copy in copies:
            copy.wait_recv()
        total = bufs[0][0]
        for j in range(1, bufs[0].shape[0]):
            total = total + bufs[0][j]
        return total

    def note(step, diag):
        spectrum[step : step + 1, :] = diag[:, :count]

    first = image[...].astype(BF16)
    copies = gram_send("col", dot(first, first, ROWS), grams[:4])
    weight = (dot(first, cp[...], ROWS) * scale).astype(BF16)

    parts = nc if lr % (128 * nc) == 0 else 1
    span = lr // parts
    exchange = []

    def middle(part):
        acc[:, part] = dot(first, tile[part, :], ROWS)

    loop(lr, 256, middle)
    hand_all("land")
    for copy in direct + across:
        copy.wait_recv()

    for p in range(parts):
        low = p * span
        value = acc[:, low : low + span] + dot(weight, rp[:, low : low + span])
        cs_land[p, col] = value.astype(BF16)
        for d, peer in enumerate(col_peers):
            mine = cs_land.at[p, col]
            exchange.append(remote(mine, mine, s_cs.at[d, p], r_cs.at[d, p], {"col": peer}))
            exchange[-1].start()
    started.extend(exchange)
    inverse, diag = cholesky_inverse(gram_take(copies, grams[:4]), count)
    note(0, diag)
    for p in range(parts):
        for copy in exchange[p * (nc - 1) : (p + 1) * (nc - 1)]:
            copy.wait_recv()
        block = cs_land[p, 0].astype(F32)
        for j in range(1, nc):
            block = block + cs_land[p, j].astype(F32)
        value = dot(inverse, block, precision=lax.Precision.HIGHEST)
        vec[:, p * span : (p + 1) * span] = value.astype(BF16)

    second = vec[...]
    copies = gram_send("row", dot(second, second, ROWS), grams[4:8])
    weight = (dot(second, rp[...], ROWS) * scale).astype(BF16)

    length = lc // nr
    if length % 128 == 0:

        def make(k):
            part = pl.ds(pl.multiple_of(k * length, 128), length)
            return dot(vec[...], tile[:, part]) + dot(weight, cp[:, part])

    else:
        make = None

        def final(part):
            acc[:, part] = dot(vec[...], tile[:, part]) + dot(weight, cp[:, part])

        loop(lc, 512, final)
    kept = []

    def factor_second():
        kept.extend(cholesky_inverse(gram_take(copies, grams[4:8]), count))

    for _ in row_sum(sums_b, factor_second, make):
        pass
    inverse, diag = kept
    note(1, diag)
    blocks = [(h, j) for h in range(2) for j in range(nz)]
    ready = sums_b[5]
    gram = jnp.zeros((height, height), F32)
    for h, j in blocks:
        gram = gram + dot(ready[h, j], ready[h, j], ROWS)
    copies = gram_send("col", gram, grams[8:12])
    exact = lax.Precision.HIGHEST
    gram = dot(inverse, gram_take(copies, grams[8:12]), precision=exact)
    gram = dot(gram, inverse, ROWS, precision=exact)
    last, diag = cholesky_inverse(gram, count)
    note(2, diag)
    turn = dot(last, inverse, precision=exact) * root
    coarse = turn.astype(BF16)
    stack = jnp.concatenate([coarse, (turn - coarse.astype(F32)).astype(BF16)], axis=0)
    for h, j in blocks:
        low = (h * nz + j) * length
        value = dot(stack, ready[h, j])
        pcs[:, low : low + length] = (value[:height] + value[height:])[:count]

    for copy in by_col + by_row + across + direct + started:
        copy.wait_send()
    for s in range(nr - 1):
        for e in range(groups + 1):
            to_right, to_left = sends(s, e)

            @pl.when(to_right)
            def _():
                rightward(s, e).wait_send()

            @pl.when(to_left)
            def _():
                leftward(s, e).wait_send()

    hand_all("drain")


def main_call(genotypes, snp_index, freq_table, prior, start):
    nr, nc = lax.axis_size("row"), lax.axis_size("col")
    own, samples = genotypes.shape
    depth = own * nr * nc
    lr, lc = prior.shape
    count = start.shape[0]
    height = -(-count // HEIGHT) * HEIGHT
    groups = min(nc, 4)
    nz = nr // 2
    length = lc // nr
    dma = pltpu.SemaphoreType.DMA
    vmem = pl.BlockSpec(memory_space=pltpu.VMEM)
    hbm = pl.BlockSpec(memory_space=pltpu.HBM)
    band = min(128, lr)

    def sum_scratch():
        return [
            pltpu.VMEM((2, nz, height, length), BF16),
            pltpu.VMEM((nz, height, length), BF16),
            pltpu.VMEM((nz - 1, height, length), BF16),
            pltpu.VMEM((nz - 1, height, length), BF16),
            pltpu.VMEM((height, length), BF16),
            pltpu.VMEM((2, nz, height, length), BF16),
            dma((nz,)),
            dma((nz,)),
            dma((nz - 1,)),
            dma((nz - 1,)),
            dma((nz - 1,)),
            dma((nz - 1,)),
            dma((nz,)),
            dma((nz,)),
        ]

    def gram_scratch(n):
        return [
            pltpu.VMEM((n, height, height), F32),
            pltpu.VMEM((height, height), F32),
            dma((n - 1,)),
            dma((n - 1,)),
        ]

    one = nr - 1 if nc <= 4 else 1
    scratch = [
        pltpu.SMEM((own,), jnp.int32),
        pltpu.SMEM(freq_table.shape, F32),
        pltpu.VMEM((count, lr), F32),
        pltpu.VMEM((own, samples), jnp.int32),
        pltpu.VMEM((own, samples), BF16),
        pltpu.VMEM((SLOTS, band, lc), F32),
        pltpu.VMEM((height, lc), F32),
        pltpu.VMEM((height, lr), BF16),
        pltpu.VMEM((height, lc), F32),
        pltpu.VMEM((lc // lr, height, lr), BF16),
        pltpu.VMEM((nc, height, depth), BF16),
        dma((SLOTS,)),
        dma((4,)),
        dma((nr - 1,)),
        dma((nr - 1,)),
        dma((nc - 1,)),
        dma((nc - 1,)),
        dma((nc - 1, nr)),
        dma((nc - 1, nr)),
    ]
    scratch += [dma((nr - 1, groups + 1))] * 4
    scratch += sum_scratch() + sum_scratch()
    parts = nc if lr % (128 * nc) == 0 else 1
    scratch += [pltpu.VMEM((parts, nc, height, lr // parts), BF16)]
    scratch += [dma((nc - 1, parts))] * 2
    scratch += [dma((nc - 1,))] * 4
    scratch += [dma((one, groups, 2))] * 2 + [dma((one, groups, 2, nc - 2)), dma((one, groups, 2))]
    scratch += gram_scratch(nc) + gram_scratch(nr) + gram_scratch(nc)
    args = (snp_index, freq_table, genotypes, start, prior)
    return pl.pallas_call(
        functools.partial(main_kernel, nr, nc, count, float(samples) ** 0.5),
        in_specs=[hbm] * 5,
        out_specs=[vmem] * 5,
        out_shape=[
            jax.ShapeDtypeStruct((depth, lr), BF16),
            jax.ShapeDtypeStruct((depth, lc), BF16),
            jax.ShapeDtypeStruct((lr, lc), BF16),
            jax.ShapeDtypeStruct((count, lc), F32),
            jax.ShapeDtypeStruct((ITERS, count), F32),
        ],
        scratch_shapes=scratch,
        compiler_params=pltpu.CompilerParams(
            collective_id=20, has_side_effects=True, vmem_limit_bytes=22 * 2**20
        ),
        name="main",
    )(*[pltpu.with_memory_space_constraint(x, pltpu.HBM) for x in args])


def tile_kernel(scale, rows_ref, cols_ref, prior_ref, pcs_ref, spectrum_ref, grm_ref, v_ref, d_ref):
    @pl.when(pl.program_id(0) == 0)
    def _():
        v_ref[...] = pcs_ref[...]
        d_ref[...] = spectrum_ref[...]

    def part(cut):
        window = dot(rows_ref[...], cols_ref[:, cut], ((0,), (0,)))
        grm_ref[:, cut] = prior_ref[:, cut].astype(F32) + window * scale

    step = min(512, cols_ref.shape[1])
    for low in range(0, cols_ref.shape[1], step):
        part(slice(low, low + step))


def make_tile(row_panel, col_panel, prior, pcs, spectrum):
    depth = row_panel.shape[0]
    rows, cols = prior.shape
    bm = min(256, rows)
    return pl.pallas_call(
        functools.partial(tile_kernel, 1.0 / depth),
        grid=(rows // bm,),
        in_specs=[
            pl.BlockSpec((depth, bm), lambda i: (0, i)),
            pl.BlockSpec((depth, cols), lambda i: (0, 0)),
            pl.BlockSpec((bm, cols), lambda i: (i, 0)),
            pl.BlockSpec(pcs.shape, lambda i: (0, 0)),
            pl.BlockSpec(spectrum.shape, lambda i: (0, 0)),
        ],
        out_specs=[
            pl.BlockSpec((bm, cols), lambda i: (i, 0)),
            pl.BlockSpec(pcs.shape, lambda i: (0, 0)),
            pl.BlockSpec(spectrum.shape, lambda i: (0, 0)),
        ],
        out_shape=[
            jax.ShapeDtypeStruct((rows, cols), F32),
            jax.ShapeDtypeStruct(pcs.shape, F32),
            jax.ShapeDtypeStruct(spectrum.shape, F32),
        ],
        compiler_params=pltpu.CompilerParams(
            dimension_semantics=("arbitrary",), vmem_limit_bytes=24 * 2**20
        ),
        cost_estimate=pl.CostEstimate(
            flops=2 * rows * cols * depth, bytes_accessed=6 * rows * cols, transcendentals=0
        ),
        name="tile",
    )(row_panel, col_panel, prior, pcs, spectrum)


def body(genotypes, snp_index, freq_table, prior, start_vectors):
    row_panel, col_panel, tile, pcs, spectrum = main_call(
        genotypes, snp_index, freq_table, prior, start_vectors.T
    )
    grm, pcs, spectrum = make_tile(row_panel, col_panel, tile, pcs, spectrum)
    return grm, pcs.T, spectrum


def solution(mesh):
    return jax.shard_map(
        body,
        mesh=mesh,
        in_specs=(P(("row", "col"), None), P(("row", "col")), P(), P("row", "col"), P("row", None)),
        out_specs=(P("row", "col"), P("col", None), P()),
        check_vma=False,
    )
```
